32 devices in a mesh: pod: 1 (over z), data: 4 (over y), tensor: 8 (over x, core).
Axes of the slice: x: 4, y: 4, z: 1, core: 2. Of those that a mesh axis runs over, the one named last changes fastest.
The devices are a block of a 4x4x8 slice.
Arguments:
- token_ids: int32 [32768], P(('pod', 'data'))
- embed_table: bfloat16 [50304, 768], P('tensor')
- norm_gain: bfloat16 [768], replicated
- w_in: bfloat16 [768, 3072], P(None, 'tensor')
- w_out: bfloat16 [3072, 768], P('tensor')
- d_out: bfloat16 [32768, 768], P(('pod', 'data', 'tensor'))
Outputs:
- output 1: bfloat16 [32768, 768], P(('pod', 'data', 'tensor'))
- output 2: float32 [50304, 768], P(('pod', 'tensor'))
- output 3: float32 [768, 3072], P('pod', 'tensor')
- output 4: float32 [3072, 768], P(('pod', 'tensor'))
All inputs are finite; a program needn't handle non-finite values.
Results may differ from the reference program's by a relative error of at most 0.0057936.
Values are sent between devices in bfloat16 or wider.
A program may use at most 768 MiB of HBM per device.

```python
import jax
import jax.numpy as jnp
from jax import lax

DATA_WAYS = 4
TENSOR_WAYS = 8
TOK_DEV = 1024
VOCAB_SIZE = 50304
MODEL_DIM = 768
FFN_DIM = 3072
NORM_EPS = 1e-6
TOKENS_REP = TOK_DEV * TENSOR_WAYS


def gelu_tanh(value):
    return jax.nn.gelu(value, approximate=True)


def draw_ids(id_key):
    k_base, k_shift, k_hot, k_pick, k_use = jax.random.split(id_key, 5)
    total_tok = DATA_WAYS * TOKENS_REP
    base_ids = jax.random.randint(k_base, (total_tok,), 0, VOCAB_SIZE)
    shift_by = jax.random.randint(k_shift, (total_tok,), 0, 3)
    skewed = jnp.right_shift(base_ids, shift_by)
    hot_ids = jax.random.randint(k_hot, (16,), 0, VOCAB_SIZE)
    hot_pick = jax.random.randint(k_pick, (total_tok,), 0, 16)
    use_hot = jax.random.randint(k_use, (total_tok,), 0, 4) == 0
    token_ids = jnp.where(use_hot, hot_ids[hot_pick], skewed)
    token_ids = token_ids.at[0].set(0).at[total_tok - 1].set(VOCAB_SIZE - 1)
    return token_ids.astype(jnp.int32)


def setup_inputs(seed: int = 0, part: int = 0) -> dict:
    root_key = jax.random.key(seed)
    k_table, k_gain, k_in, k_out, k_part = jax.random.split(root_key, 5)
    k_ids, k_grad = jax.random.split(jax.random.fold_in(k_part, part))
    total_tok = DATA_WAYS * TOKENS_REP
    embed_table = jax.random.normal(k_table, (VOCAB_SIZE, MODEL_DIM), jnp.float32).astype(jnp.bfloat16)
    norm_gain = (1.0 + 0.5 * jax.random.uniform(k_gain, (MODEL_DIM,), jnp.float32, -1.0, 1.0)).astype(jnp.bfloat16)
    w_in = (jax.random.normal(k_in, (MODEL_DIM, FFN_DIM), jnp.float32) * MODEL_DIM ** -0.5).astype(jnp.bfloat16)
    w_out = (jax.random.normal(k_out, (FFN_DIM, MODEL_DIM), jnp.float32) * (1.5 * FFN_DIM ** -0.5)).astype(jnp.bfloat16)
    d_out = jax.random.normal(k_grad, (total_tok, MODEL_DIM), jnp.float32).astype(jnp.bfloat16)
    return {"token_ids": draw_ids(k_ids), "embed_table": embed_table, "norm_gain": norm_gain, "w_in": w_in, "w_out": w_out, "d_out": d_out}


def reference(token_ids, embed_table, norm_gain, w_in, w_out, d_out):
    blocks = DATA_WAYS * TENSOR_WAYS
    embedded = jnp.take(embed_table, token_ids, axis=0).reshape(blocks, TOK_DEV, MODEL_DIM)
    grad_blocks = d_out.reshape(blocks, TOK_DEV, MODEL_DIM)
    gain_f32 = norm_gain.astype(jnp.float32)

    def block_step(acc_pair, step_in):
        acc_w_in, acc_w_out = acc_pair
        x_blk, dy_blk = step_in
        x_f32 = x_blk.astype(jnp.float32)
        inv_rms = lax.rsqrt(jnp.mean(x_f32 * x_f32, axis=-1, keepdims=True) + NORM_EPS)
        x_hat = x_f32 * inv_rms
        normed = (x_hat * gain_f32).astype(jnp.bfloat16)
        pre_gelu = jnp.dot(normed, w_in, preferred_element_type=jnp.float32).astype(jnp.bfloat16)
        hidden_f32, gelu_pull = jax.vjp(gelu_tanh, pre_gelu.astype(jnp.float32))
        hidden = hidden_f32.astype(jnp.bfloat16)
        mlp_out = jnp.dot(hidden, w_out, preferred_element_type=jnp.float32)
        out_blk = (x_f32 + mlp_out).astype(jnp.bfloat16)
        grad_hidden = jnp.dot(dy_blk, w_out.T, preferred_element_type=jnp.float32)
        grad_pre = gelu_pull(grad_hidden)[0].astype(jnp.bfloat16)
        acc_w_out = acc_w_out + jnp.dot(hidden.T, dy_blk, preferred_element_type=jnp.float32)
        acc_w_in = acc_w_in + jnp.dot(normed.T, grad_pre, preferred_element_type=jnp.float32)
        d_normed = jnp.dot(grad_pre, w_in.T, preferred_element_type=jnp.float32)
        d_hat = d_normed * gain_f32
        d_norm_in = inv_rms * (d_hat - x_hat * jnp.mean(d_hat * x_hat, axis=-1, keepdims=True))
        dx_blk = (dy_blk.astype(jnp.float32) + d_norm_in).astype(jnp.bfloat16)
        return (acc_w_in, acc_w_out), (out_blk, dx_blk)

    zeros_in = jnp.zeros((MODEL_DIM, FFN_DIM), jnp.float32)
    zeros_out = jnp.zeros((FFN_DIM, MODEL_DIM), jnp.float32)
    (grad_w_in, grad_w_out), (out_blocks, dx_blocks) = lax.scan(block_step, (zeros_in, zeros_out), (embedded, grad_blocks))
    grad_table = jax.ops.segment_sum(dx_blocks.reshape(-1, MODEL_DIM).astype(jnp.float32), token_ids, num_segments=VOCAB_SIZE)
    return out_blocks.reshape(-1, MODEL_DIM), grad_table, grad_w_in, grad_w_out
```

```python
import functools

import jax
import jax.numpy as jnp
from jax import lax
from jax.experimental import pallas as pl
from jax.experimental.pallas import tpu as pltpu
from jax.sharding import PartitionSpec as P

NORM_EPS = 1e-6
HALVES = 2
F32 = jnp.float32
BF16 = jnp.bfloat16
NT = (((1,), (1,)), ((), ()))
TN = (((0,), (0,)), ((), ()))


def gelu_tanh(value):
    return jax.nn.gelu(value, approximate=True)


def list_kernel(rows, bits, per_part, n_parts, base_ref, ids_ref, list_ref):
    base = base_ref[0]
    n_tok = per_part * n_parts

    def one_part(part, count):
        list_ref[n_tok + part] = count

        def one_token(pos, count):
            local = ids_ref[part * per_part + pos] - base
            list_ref[count] = (pos << bits) | (local & ((1 << bits) - 1))
            owned = jnp.logical_and(local >= 0, local < rows)
            return count + owned.astype(jnp.int32)

        return lax.fori_loop(0, per_part, one_token, count, unroll=16)

    list_ref[n_tok + n_parts] = lax.fori_loop(0, n_parts, one_part, jnp.int32(0))


def list_owned(token_ids, rows, rank, n_parts):
    n_tok = token_ids.shape[0]
    bits = rows.bit_length()
    size = n_tok + 128
    return pl.pallas_call(
        functools.partial(list_kernel, rows, bits, n_tok // n_parts, n_parts),
        out_shape=jax.ShapeDtypeStruct((size,), jnp.int32),
        in_specs=[pl.BlockSpec(memory_space=pltpu.SMEM)] * 2,
        out_specs=pl.BlockSpec(memory_space=pltpu.SMEM),
        cost_estimate=pl.CostEstimate(flops=n_tok * 4000, bytes_accessed=8 * n_tok, transcendentals=0),
    )((rank * rows)[None].astype(jnp.int32), token_ids)


def scatter_kernel(bits, n_dev, half, n_tok, size, list_ref, part_ref, *refs):
    out_ref, table, stage, sem = refs[-4:]
    step = pl.program_id(0)
    rows = table.shape[0]
    tile = 8

    @pl.when(step == 0)
    def _():
        if len(refs) > 4:
            copy = pltpu.make_async_copy(refs[0], table, sem)
            copy.start()
            copy.wait()
        else:

            def clear(i, carry):
                table[pl.ds(pl.multiple_of(i * tile, tile), tile), :] = jnp.zeros((tile, table.shape[1]), F32)
                return carry

            lax.fori_loop(0, rows // tile, clear, 0, unroll=2)

    stage[...] = part_ref[...].astype(F32)

    replica = step // n_dev
    dev = step - replica * n_dev
    base = replica * size
    first = list_ref[base + n_tok + dev * HALVES + half]
    last = list_ref[base + n_tok + dev * HALVES + half + 1]
    mask = (1 << bits) - 1

    def add(k):
        entry = list_ref[base + k]
        pos = entry >> bits
        row = entry & mask
        table[pl.ds(row, 1), :] = table[pl.ds(row, 1), :] + stage[pl.ds(pos, 1), :]

    n_quads = (last - first) >> 2

    def quad(i, carry):
        for j in range(4):
            add(first + i * 4 + j)
        return carry

    lax.fori_loop(0, n_quads, quad, 0)

    def single(k, carry):
        add(k)
        return carry

    lax.fori_loop(first + n_quads * 4, last, single, 0)

    @pl.when(step == pl.num_programs(0) - 1)
    def _():
        copy = pltpu.make_async_copy(table, out_ref, sem)
        copy.start()
        copy.wait()


def scatter_rows(lists, part, half, table, rows, n_dev, n_rep):
    size = lists.shape[0] // n_rep
    total, dim = part.shape
    per_part = total // (n_dev * n_rep)
    n_tok = per_part * HALVES * n_dev
    more = [] if table is None else [table]
    return pl.pallas_call(
        functools.partial(scatter_kernel, rows.bit_length(), n_dev, half, n_tok, size),
        out_shape=jax.ShapeDtypeStruct((rows, dim), F32),
        grid_spec=pltpu.PrefetchScalarGridSpec(
            num_scalar_prefetch=1,
            grid=(n_dev * n_rep,),
            in_specs=[pl.BlockSpec((per_part, dim), lambda i, *_: (i, 0))] + [pl.BlockSpec(memory_space=pl.ANY)] * len(more),
            out_specs=pl.BlockSpec(memory_space=pl.ANY),
            scratch_shapes=[
                pltpu.VMEM((rows, dim), F32),
                pltpu.VMEM((per_part, dim), F32),
                pltpu.SemaphoreType.DMA,
            ],
        ),
        input_output_aliases={2: 0} if more else {},
        compiler_params=pltpu.CompilerParams(vmem_limit_bytes=32 << 20, dimension_semantics=("arbitrary",)),
        cost_estimate=pl.CostEstimate(
            flops=total * 1000000, bytes_accessed=8 * rows * dim + 2 * total * dim, transcendentals=0
        ),
    )(lists, part, *more)


def solution(mesh):
    tok_spec = P(("pod", "data", "tensor"), None)
    n_dev = mesh.shape["tensor"]
    n_rep = mesh.shape["data"]

    def body(token_ids, embed_table, norm_gain, w_in, w_out, d_out):
        shard_rows, _ = embed_table.shape
        rank = lax.axis_index("tensor")
        replica = lax.axis_index("data")
        n_tok = token_ids.shape[0]
        per_dev = n_tok // n_dev
        half = per_dev // HALVES

        piece = w_out.shape[0] // n_rep
        both = ("tensor", "data")
        w2 = lax.all_gather(lax.dynamic_slice_in_dim(w_out, replica * piece, piece), both, axis=0, tiled=True)
        w1t = lax.all_gather(lax.dynamic_slice_in_dim(w_in.T, replica * piece, piece), both, axis=0, tiled=True)

        ids_by_dev = token_ids.reshape(n_dev, HALVES, half)
        gain_f32 = norm_gain.astype(F32)

        x_halves = []
        for k in range(HALVES):
            local_ids = ids_by_dev[:, k].reshape(-1) - rank * shard_rows
            is_owned = (local_ids >= 0) & (local_ids < shard_rows)
            picked = jnp.take(embed_table, jnp.where(is_owned, local_ids, 0), axis=0)
            partial_rows = jnp.where(is_owned[:, None], picked, jnp.zeros_like(picked))
            x_halves.append(lax.psum_scatter(partial_rows, "tensor", scatter_dimension=0, tiled=True))

        lists = list_owned(token_ids, shard_rows, rank, n_dev * HALVES)
        lists = lax.all_gather(lists, "data", axis=0, tiled=True)

        outs, grads, saved = [], [], []
        for k in range(HALVES):
            x_half = x_halves[k]
            if k > 0:
                x_half, _ = lax.optimization_barrier((x_half, d_embed))
            x_f32 = x_half.astype(F32)
            d_half = lax.slice_in_dim(d_out, k * half, (k + 1) * half)
            inv_rms = lax.rsqrt(jnp.mean(x_f32 * x_f32, axis=-1, keepdims=True) + NORM_EPS)
            x_hat = x_f32 * inv_rms
            normed = (x_hat * gain_f32).astype(BF16)
            pre_gelu = lax.dot_general(normed, w1t, NT, preferred_element_type=F32).astype(BF16)
            hidden_f32, gelu_pull = jax.vjp(gelu_tanh, pre_gelu.astype(F32))
            hidden = hidden_f32.astype(BF16)
            grad_hidden = lax.dot_general(d_half, w2, NT, preferred_element_type=F32)
            grad_pre = gelu_pull(grad_hidden)[0].astype(BF16)
            d_normed = jnp.dot(grad_pre, w1t, preferred_element_type=F32)
            d_hat = d_normed * gain_f32
            d_norm_in = inv_rms * (d_hat - x_hat * jnp.mean(d_hat * x_hat, axis=-1, keepdims=True))
            d_embed = (d_half.astype(F32) + d_norm_in).astype(BF16)
            grads.append(lax.all_gather(d_embed, ("data", "tensor"), axis=0, tiled=True))
            normed, hidden, grad_pre, d_half, _ = lax.optimization_barrier((normed, hidden, grad_pre, d_half, d_embed))
            saved.append((normed, hidden, grad_pre, d_half))
            mlp_out = jnp.dot(hidden, w2, preferred_element_type=F32)
            outs.append((x_f32 + mlp_out).astype(BF16))
        block_out = jnp.concatenate(outs, axis=0)

        grad_w2 = sum(lax.dot_general(h, d, TN, preferred_element_type=F32) for _, h, _, d in saved)
        grad_w1t = sum(lax.dot_general(u, n, TN, preferred_element_type=F32) for n, _, u, _ in saved)
        grad_w2 = lax.psum_scatter(grad_w2, both, scatter_dimension=0, tiled=True)
        grad_w1t = lax.psum_scatter(grad_w1t, both, scatter_dimension=0, tiled=True)
        grad_w2 = lax.all_gather(grad_w2, "data", axis=0, tiled=True)
        grad_w1t = lax.all_gather(grad_w1t, "data", axis=0, tiled=True)

        grad_table = None
        for k in range(HALVES):
            grad_table = scatter_rows(lists, grads[k], k, grad_table, shard_rows, n_dev, n_rep)
        return block_out, grad_table, grad_w1t.T, grad_w2

    return jax.shard_map(
        body,
        mesh=mesh,
        in_specs=(P(("pod", "data")), P("tensor", None), P(None), P(None, "tensor"), P("tensor", None), tok_spec),
        out_specs=(tok_spec, P(("pod", "tensor"), None), P("pod", "tensor"), P(("pod", "tensor"), None)),
        check_vma=False,
    )
```

```python
import functools

import jax
import jax.numpy as jnp
from jax import lax
from jax.experimental import pallas as pl
from jax.experimental.layout import Layout, with_layout_constraint
from jax.experimental.pallas import tpu as pltpu
from jax.sharding import PartitionSpec as P

NORM_EPS = 1e-6
HALVES = 2
F32 = jnp.float32
BF16 = jnp.bfloat16
NT = (((1,), (1,)), ((), ()))
TN = (((0,), (0,)), ((), ()))


def gelu_tanh(value):
    return jax.nn.gelu(value, approximate=True)


def list_kernel(rows, bits, per_part, n_parts, base_ref, ids_ref, list_ref):
    base = base_ref[0]
    n_tok = per_part * n_parts

    def one_part(part, count):
        list_ref[n_tok + part] = count

        def one_token(pos, count):
            local = ids_ref[part * per_part + pos] - base
            list_ref[count] = (pos << bits) | (local & ((1 << bits) - 1))
            owned = jnp.logical_and(local >= 0, local < rows)
            return count + owned.astype(jnp.int32)

        return lax.fori_loop(0, per_part, one_token, count, unroll=16)

    list_ref[n_tok + n_parts] = lax.fori_loop(0, n_parts, one_part, jnp.int32(0))


def list_owned(token_ids, rows, rank, n_parts):
    n_tok = token_ids.shape[0]
    bits = rows.bit_length()
    size = n_tok + 128
    return pl.pallas_call(
        functools.partial(list_kernel, rows, bits, n_tok // n_parts, n_parts),
        out_shape=jax.ShapeDtypeStruct((size,), jnp.int32),
        in_specs=[pl.BlockSpec(memory_space=pltpu.SMEM)] * 2,
        out_specs=pl.BlockSpec(memory_space=pltpu.SMEM),
        cost_estimate=pl.CostEstimate(flops=n_tok * 4000, bytes_accessed=8 * n_tok, transcendentals=0),
    )((rank * rows)[None].astype(jnp.int32), token_ids)


def scatter_kernel(bits, n_dev, n_tok, size, list_ref, part_ref, out_ref, table, stage, sem):
    step = pl.program_id(0)
    rows = table.shape[0]
    tile = 8

    @pl.when(step == 0)
    def _():
        def clear(i, carry):
            table[pl.ds(pl.multiple_of(i * tile, tile), tile), :] = jnp.zeros((tile, table.shape[1]), F32)
            return carry

        lax.fori_loop(0, rows // tile, clear, 0, unroll=2)

    stage[...] = part_ref[...].astype(F32)

    replica = step // n_dev
    dev = step - replica * n_dev
    base = replica * size
    first = list_ref[base + n_tok + dev]
    last = list_ref[base + n_tok + dev + 1]
    mask = (1 << bits) - 1

    def add(k):
        entry = list_ref[base + k]
        pos = entry >> bits
        row = entry & mask
        table[pl.ds(row, 1), :] = table[pl.ds(row, 1), :] + stage[pl.ds(pos, 1), :]

    n_quads = (last - first) >> 2

    def quad(i, carry):
        for j in range(4):
            add(first + i * 4 + j)
        return carry

    lax.fori_loop(0, n_quads, quad, 0)

    def single(k, carry):
        add(k)
        return carry

    lax.fori_loop(first + n_quads * 4, last, single, 0)

    @pl.when(step == pl.num_programs(0) - 1)
    def _():
        copy = pltpu.make_async_copy(table, out_ref, sem)
        copy.start()
        copy.wait()


def scatter_rows(lists, part, rows, n_dev, n_rep):
    size = lists.shape[0] // n_rep
    total, dim = part.shape
    per_part = total // (n_dev * n_rep)
    n_tok = per_part * n_dev
    return pl.pallas_call(
        functools.partial(scatter_kernel, rows.bit_length(), n_dev, n_tok, size),
        out_shape=jax.ShapeDtypeStruct((rows, dim), F32),
        grid_spec=pltpu.PrefetchScalarGridSpec(
            num_scalar_prefetch=1,
            grid=(n_dev * n_rep,),
            in_specs=[pl.BlockSpec((per_part, dim), lambda i, *_: (i, 0))],
            out_specs=pl.BlockSpec(memory_space=pl.ANY),
            scratch_shapes=[
                pltpu.VMEM((rows, dim), F32),
                pltpu.VMEM((per_part, dim), F32),
                pltpu.SemaphoreType.DMA,
            ],
        ),
        compiler_params=pltpu.CompilerParams(vmem_limit_bytes=32 << 20, dimension_semantics=("arbitrary",)),
        cost_estimate=pl.CostEstimate(
            flops=total * 1000000, bytes_accessed=4 * rows * dim + 2 * total * dim, transcendentals=0
        ),
    )(lists, part)


def solution(mesh):
    tok_spec = P(("pod", "data", "tensor"), None)
    n_dev = mesh.shape["tensor"]
    n_rep = mesh.shape["data"]

    def body(token_ids, embed_table, norm_gain, w_in, w_out, d_out):
        shard_rows, _ = embed_table.shape
        rank = lax.axis_index("tensor")
        n_tok = token_ids.shape[0]
        per_dev = n_tok // n_dev
        half = per_dev // HALVES

        w1t = with_layout_constraint(w_in.T, Layout(major_to_minor=(0, 1)))
        w1t = lax.all_gather(w1t, "tensor", axis=0, tiled=True)
        w2 = lax.all_gather(w_out, "tensor", axis=0, tiled=True)

        ids_by_dev = token_ids.reshape(n_dev, HALVES, half)
        gain_f32 = norm_gain.astype(F32)

        x_halves = []
        for k in range(HALVES):
            local_ids = ids_by_dev[:, k].reshape(-1) - rank * shard_rows
            is_owned = (local_ids >= 0) & (local_ids < shard_rows)
            picked = jnp.take(embed_table, jnp.where(is_owned, local_ids, 0), axis=0)
            partial_rows = jnp.where(is_owned[:, None], picked, jnp.zeros_like(picked))
            x_halves.append(lax.psum_scatter(partial_rows, "tensor", scatter_dimension=0, tiled=True))

        lists = list_owned(token_ids, shard_rows, rank, n_dev)
        lists = lax.all_gather(lists, "data", axis=0, tiled=True)

        outs, grads, saved = [], [], []
        for k in range(HALVES):
            x_half = x_halves[k]
            if k > 0:
                x_half, _ = lax.optimization_barrier((x_half, d_embed))
            x_f32 = x_half.astype(F32)
            d_half = lax.slice_in_dim(d_out, k * half, (k + 1) * half)
            inv_rms = lax.rsqrt(jnp.mean(x_f32 * x_f32, axis=-1, keepdims=True) + NORM_EPS)
            x_hat = x_f32 * inv_rms
            normed = (x_hat * gain_f32).astype(BF16)
            pre_gelu = lax.dot_general(normed, w1t, NT, preferred_element_type=F32).astype(BF16)
            hidden_f32, gelu_pull = jax.vjp(gelu_tanh, pre_gelu.astype(F32))
            hidden = hidden_f32.astype(BF16)
            grad_hidden = lax.dot_general(d_half, w2, NT, preferred_element_type=F32)
            grad_pre = gelu_pull(grad_hidden)[0].astype(BF16)
            d_normed = jnp.dot(grad_pre, w1t, preferred_element_type=F32)
            d_hat = d_normed * gain_f32
            d_norm_in = inv_rms * (d_hat - x_hat * jnp.mean(d_hat * x_hat, axis=-1, keepdims=True))
            d_embed = (d_half.astype(F32) + d_norm_in).astype(BF16)
            grads.append(d_embed)
            normed, hidden, grad_pre, d_half, _ = lax.optimization_barrier((normed, hidden, grad_pre, d_half, d_embed))
            saved.append((normed, hidden, grad_pre, d_half))
            mlp_out = jnp.dot(hidden, w2, preferred_element_type=F32)
            outs.append((x_f32 + mlp_out).astype(BF16))
        block_out = jnp.concatenate(outs, axis=0)
        grad_all = lax.all_gather(jnp.concatenate(grads, axis=0), ("data", "tensor"), axis=0, tiled=True)

        grad_w2 = sum(lax.dot_general(h, d, TN, preferred_element_type=F32) for _, h, _, d in saved)
        grad_w1t = sum(lax.dot_general(u, n, TN, preferred_element_type=F32) for n, _, u, _ in saved)
        grad_w2 = lax.psum_scatter(grad_w2, "tensor", scatter_dimension=0, tiled=True)
        grad_w1t = lax.psum_scatter(grad_w1t, "tensor", scatter_dimension=0, tiled=True)
        grad_w2, grad_w1t = lax.psum((grad_w2, grad_w1t), "data")
        grad_table = scatter_rows(lists, grad_all, shard_rows, n_dev, n_rep)
        return block_out, grad_table, grad_w1t.T, grad_w2

    return jax.shard_map(
        body,
        mesh=mesh,
        in_specs=(P(("pod", "data")), P("tensor", None), P(None), P(None, "tensor"), P("tensor", None), tok_spec),
        out_specs=(tok_spec, P(("pod", "tensor"), None), P("pod", "tensor"), P(("pod", "tensor"), None)),
        check_vma=False,
    )
```

```python
import functools

import jax
import jax.numpy as jnp
from jax import lax
from jax.experimental import pallas as pl
from jax.experimental.layout import Layout, with_layout_constraint
from jax.experimental.pallas import tpu as pltpu
from jax.sharding import PartitionSpec as P

NORM_EPS = 1e-6
HALVES = 2
F32 = jnp.float32
BF16 = jnp.bfloat16
NT = (((1,), (1,)), ((), ()))
TN = (((0,), (0,)), ((), ()))


def gelu_tanh(value):
    return jax.nn.gelu(value, approximate=True)


def list_kernel(rows, bits, per_part, n_parts, base_ref, ids_ref, list_ref):
    base = base_ref[0]
    n_tok = per_part * n_parts

    def one_part(part, count):
        list_ref[n_tok + part] = count

        def one_token(pos, count):
            local = ids_ref[part * per_part + pos] - base
            list_ref[count] = (pos << bits) | (local & ((1 << bits) - 1))
            owned = jnp.logical_and(local >= 0, local < rows)
            return count + owned.astype(jnp.int32)

        return lax.fori_loop(0, per_part, one_token, count, unroll=16)

    list_ref[n_tok + n_parts] = lax.fori_loop(0, n_parts, one_part, jnp.int32(0))


def list_owned(token_ids, rows, rank, n_parts):
    n_tok = token_ids.shape[0]
    bits = rows.bit_length()
    size = n_tok + 128
    return pl.pallas_call(
        functools.partial(list_kernel, rows, bits, n_tok // n_parts, n_parts),
        out_shape=jax.ShapeDtypeStruct((size,), jnp.int32),
        in_specs=[pl.BlockSpec(memory_space=pltpu.SMEM)] * 2,
        out_specs=pl.BlockSpec(memory_space=pltpu.SMEM),
        cost_estimate=pl.CostEstimate(flops=n_tok * 4000, bytes_accessed=8 * n_tok, transcendentals=0),
    )((rank * rows)[None].astype(jnp.int32), token_ids)


def scatter_kernel(bits, n_dev, n_tok, size, list_ref, part_ref, out_ref, table, stage, sem):
    step = pl.program_id(0)
    rows = table.shape[0]
    tile = 8

    @pl.when(step == 0)
    def _():
        def clear(i, carry):
            table[pl.ds(pl.multiple_of(i * tile, tile), tile), :] = jnp.zeros((tile, table.shape[1]), F32)
            return carry

        lax.fori_loop(0, rows // tile, clear, 0, unroll=2)

    stage[...] = part_ref[...].astype(F32)

    replica = step // n_dev
    dev = step - replica * n_dev
    base = replica * size
    first = list_ref[base + n_tok + dev]
    last = list_ref[base + n_tok + dev + 1]
    mask = (1 << bits) - 1

    def add(k):
        entry = list_ref[base + k]
        pos = entry >> bits
        row = entry & mask
        table[pl.ds(row, 1), :] = table[pl.ds(row, 1), :] + stage[pl.ds(pos, 1), :]

    n_quads = (last - first) >> 2

    def quad(i, carry):
        for j in range(4):
            add(first + i * 4 + j)
        return carry

    lax.fori_loop(0, n_quads, quad, 0)

    def single(k, carry):
        add(k)
        return carry

    lax.fori_loop(first + n_quads * 4, last, single, 0)

    @pl.when(step == pl.num_programs(0) - 1)
    def _():
        copy = pltpu.make_async_copy(table, out_ref, sem)
        copy.start()
        copy.wait()


def scatter_rows(lists, part, rows, n_dev, n_rep):
    size = lists.shape[0] // n_rep
    total, dim = part.shape
    per_part = total // (n_dev * n_rep)
    n_tok = per_part * n_dev
    return pl.pallas_call(
        functools.partial(scatter_kernel, rows.bit_length(), n_dev, n_tok, size),
        out_shape=jax.ShapeDtypeStruct((rows, dim), F32),
        grid_spec=pltpu.PrefetchScalarGridSpec(
            num_scalar_prefetch=1,
            grid=(n_dev * n_rep,),
            in_specs=[pl.BlockSpec((per_part, dim), lambda i, *_: (i, 0))],
            out_specs=pl.BlockSpec(memory_space=pl.ANY),
            scratch_shapes=[
                pltpu.VMEM((rows, dim), F32),
                pltpu.VMEM((per_part, dim), F32),
                pltpu.SemaphoreType.DMA,
            ],
        ),
        compiler_params=pltpu.CompilerParams(vmem_limit_bytes=32 << 20, dimension_semantics=("arbitrary",)),
        cost_estimate=pl.CostEstimate(
            flops=total * 1000000, bytes_accessed=4 * rows * dim + 2 * total * dim, transcendentals=0
        ),
    )(lists, part)


def sum_kernel(n, part_ref, out_ref, parts, mine, sums, send_parts, recv_parts, send_sums, recv_sums):
    me = lax.axis_index("data")
    rows = part_ref.shape[0] // n
    peers = [lax.rem(me + k, n) for k in range(1, n)]

    barrier = pltpu.get_barrier_semaphore()
    for peer in peers:
        pl.semaphore_signal(barrier, inc=1, device_id={"data": peer}, device_id_type=pl.DeviceIdType.MESH)
    pl.semaphore_wait(barrier, n - 1)

    def piece(of):
        return pl.ds(pl.multiple_of(of * rows, 8), rows)

    def send(src, slots, k, send_sem, recv_sem):
        copy = pltpu.make_async_remote_copy(
            src_ref=src,
            dst_ref=slots.at[k],
            send_sem=send_sem.at[k],
            recv_sem=recv_sem.at[k],
            device_id={"data": peers[k]},
            device_id_type=pl.DeviceIdType.MESH,
        )
        copy.start()
        return copy

    first = [send(part_ref.at[piece(peers[k])], parts, k, send_parts, recv_parts) for k in range(n - 1)]
    total = part_ref[piece(me), :]
    for k in range(n - 1):
        first[k].wait()
        total = total + parts[k]
    mine[...] = total
    out_ref[piece(me), :] = mine[...]
    second = [send(mine, sums, k, send_sums, recv_sums) for k in range(n - 1)]
    for k in range(n - 1):
        second[k].wait()
        out_ref[piece(lax.rem(me + n - 1 - k, n)), :] = sums[k]


def sum_over_data(part, n, number):
    rows, dim = part.shape[0] // n, part.shape[1]
    sems = pltpu.SemaphoreType.DMA((n - 1,))
    return pl.pallas_call(
        functools.partial(sum_kernel, n),
        out_shape=jax.ShapeDtypeStruct(part.shape, F32),
        in_specs=[pl.BlockSpec(memory_space=pltpu.VMEM)],
        out_specs=pl.BlockSpec(memory_space=pltpu.VMEM),
        scratch_shapes=[
            pltpu.VMEM((n - 1, rows, dim), F32),
            pltpu.VMEM((rows, dim), F32),
            pltpu.VMEM((n - 1, rows, dim), F32),
            sems,
            sems,
            sems,
            sems,
        ],
        compiler_params=pltpu.CompilerParams(collective_id=number, has_side_effects=True, vmem_limit_bytes=16 << 20),
        cost_estimate=pl.CostEstimate(flops=part.size * 50000, bytes_accessed=8 * part.size, transcendentals=0),
    )(part)


def solution(mesh):
    tok_spec = P(("pod", "data", "tensor"), None)
    n_dev = mesh.shape["tensor"]
    n_rep = mesh.shape["data"]

    def body(token_ids, embed_table, norm_gain, w_in, w_out, d_out):
        shard_rows, dim = embed_table.shape
        rank = lax.axis_index("tensor")
        n_tok = token_ids.shape[0]
        per_dev = n_tok // n_dev
        half = per_dev // HALVES

        cols = w_out.shape[0]
        w_both = jnp.concatenate([w_in.T, w_out], axis=0)
        w_both = with_layout_constraint(w_both, Layout(major_to_minor=(0, 1)))
        w_both = lax.all_gather(w_both, "tensor", axis=0)
        w1t = lax.optimization_barrier(w_both[:, :cols].reshape(-1, dim))
        w2 = lax.optimization_barrier(w_both[:, cols:].reshape(-1, dim))

        ids_by_dev = token_ids.reshape(n_dev, HALVES, half)
        gain_f32 = norm_gain.astype(F32)

        x_halves = []
        for k in range(HALVES):
            local_ids = ids_by_dev[:, k].reshape(-1) - rank * shard_rows
            is_owned = (local_ids >= 0) & (local_ids < shard_rows)
            picked = jnp.take(embed_table, jnp.where(is_owned, local_ids, 0), axis=0)
            partial_rows = jnp.where(is_owned[:, None], picked, jnp.zeros_like(picked))
            x_halves.append(lax.psum_scatter(partial_rows, "tensor", scatter_dimension=0, tiled=True))

        lists = list_owned(token_ids, shard_rows, rank, n_dev)
        lists = lax.all_gather(lists, "data", axis=0, tiled=True)

        outs, grads, saved = [], [], []
        for k in range(HALVES):
            d_half = lax.slice_in_dim(d_out, k * half, (k + 1) * half)
            grad_hidden = lax.dot_general(d_half, w2, NT, preferred_element_type=F32)
            grad_hidden = lax.optimization_barrier(grad_hidden)
            x_half = x_halves[k]
            if k > 0:
                x_half, _ = lax.optimization_barrier((x_half, d_embed))
            x_f32 = x_half.astype(F32)
            inv_rms = lax.rsqrt(jnp.mean(x_f32 * x_f32, axis=-1, keepdims=True) + NORM_EPS)
            x_hat = x_f32 * inv_rms
            normed = (x_hat * gain_f32).astype(BF16)
            pre_gelu = lax.dot_general(normed, w1t, NT, preferred_element_type=F32).astype(BF16)
            hidden_f32, gelu_pull = jax.vjp(gelu_tanh, pre_gelu.astype(F32))
            hidden = hidden_f32.astype(BF16)
            grad_pre = gelu_pull(grad_hidden)[0].astype(BF16)
            d_normed = jnp.dot(grad_pre, w1t, preferred_element_type=F32)
            d_hat = d_normed * gain_f32
            d_norm_in = inv_rms * (d_hat - x_hat * jnp.mean(d_hat * x_hat, axis=-1, keepdims=True))
            d_embed = (d_half.astype(F32) + d_norm_in).astype(BF16)
            grads.append(d_embed)
            normed, hidden, grad_pre, d_half, _ = lax.optimization_barrier((normed, hidden, grad_pre, d_half, d_embed))
            saved.append((normed, hidden, grad_pre, d_half))
            mlp_out = jnp.dot(hidden, w2, preferred_element_type=F32)
            outs.append((x_f32 + mlp_out).astype(BF16))
        block_out = jnp.concatenate(outs, axis=0)
        grad_all = lax.all_gather(jnp.concatenate(grads, axis=0), ("data", "tensor"), axis=0, tiled=True)

        grad_w2 = sum(lax.dot_general(h, d, TN, preferred_element_type=F32) for _, h, _, d in saved)
        grad_w1t = sum(lax.dot_general(u, n, TN, preferred_element_type=F32) for n, _, u, _ in saved)
        grad_w2 = lax.psum_scatter(grad_w2, "tensor", scatter_dimension=0, tiled=True)
        grad_w1t = lax.psum_scatter(grad_w1t, "tensor", scatter_dimension=0, tiled=True)
        grad_w2 = sum_over_data(grad_w2, n_rep, 0)
        grad_w1t = sum_over_data(grad_w1t, n_rep, 1)
        grad_table = scatter_rows(lists, grad_all, shard_rows, n_dev, n_rep)
        return block_out, grad_table, grad_w1t.T, grad_w2

    return jax.shard_map(
        body,
        mesh=mesh,
        in_specs=(P(("pod", "data")), P("tensor", None), P(None), P(None, "tensor"), P("tensor", None), tok_spec),
        out_specs=(tok_spec, P(("pod", "tensor"), None), P("pod", "tensor"), P(("pod", "tensor"), None)),
        check_vma=False,
    )
```

```python
import functools

import jax
import jax.numpy as jnp
from jax import lax
from jax.experimental import pallas as pl
from jax.experimental.layout import Layout, with_layout_constraint
from jax.experimental.pallas import tpu as pltpu
from jax.sharding import PartitionSpec as P

NORM_EPS = 1e-6
SPLIT = (5, 3)
PAIR_ROWS = 32
F32 = jnp.float32
BF16 = jnp.bfloat16
NT = (((1,), (1,)), ((), ()))
TN = (((0,), (0,)), ((), ()))


def gelu_tanh(value):
    return jax.nn.gelu(value, approximate=True)


def list_kernel(rows, bits, per_part, n_parts, base_ref, ids_ref, list_ref):
    base = base_ref[0]
    n_tok = per_part * n_parts

    def one_part(part, count):
        list_ref[n_tok + part] = count

        def one_token(pos, count):
            local = ids_ref[part * per_part + pos] - base
            list_ref[count] = (pos << bits) | (local & ((1 << bits) - 1))
            owned = jnp.logical_and(local >= 0, local < rows)
            return count + owned.astype(jnp.int32)

        return lax.fori_loop(0, per_part, one_token, count, unroll=16)

    list_ref[n_tok + n_parts] = lax.fori_loop(0, n_parts, one_part, jnp.int32(0))


def list_owned(token_ids, rows, rank, n_parts):
    n_tok = token_ids.shape[0]
    bits = rows.bit_length()
    size = n_tok + 128
    return pl.pallas_call(
        functools.partial(list_kernel, rows, bits, n_tok // n_parts, n_parts),
        out_shape=jax.ShapeDtypeStruct((size,), jnp.int32),
        in_specs=[pl.BlockSpec(memory_space=pltpu.SMEM)] * 2,
        out_specs=pl.BlockSpec(memory_space=pltpu.SMEM),
        cost_estimate=pl.CostEstimate(flops=n_tok * 4000, bytes_accessed=8 * n_tok, transcendentals=0),
    )((rank * rows)[None].astype(jnp.int32), token_ids)


def scatter_kernel(bits, n_dev, n_tok, size, list_ref, part_ref, out_ref, table, stage, sem):
    step = pl.program_id(0)
    rows = table.shape[0]
    tile = 8

    @pl.when(step == 0)
    def _():
        def clear(i, carry):
            table[pl.ds(pl.multiple_of(i * tile, tile), tile), :] = jnp.zeros((tile, table.shape[1]), F32)
            return carry

        lax.fori_loop(0, rows // tile, clear, 0, unroll=2)

    stage[...] = part_ref[...].astype(F32)

    replica = step // n_dev
    dev = step - replica * n_dev
    base = replica * size
    first = list_ref[base + n_tok + dev]
    last = list_ref[base + n_tok + dev + 1]
    mask = (1 << bits) - 1

    def add(k):
        entry = list_ref[base + k]
        pos = entry >> bits
        row = entry & mask
        table[pl.ds(row, 1), :] = table[pl.ds(row, 1), :] + stage[pl.ds(pos, 1), :]

    n_quads = (last - first) >> 2

    def quad(i, carry):
        for j in range(4):
            add(first + i * 4 + j)
        return carry

    lax.fori_loop(0, n_quads, quad, 0)

    def single(k, carry):
        add(k)
        return carry

    lax.fori_loop(first + n_quads * 4, last, single, 0)

    @pl.when(step == pl.num_programs(0) - 1)
    def _():
        copy = pltpu.make_async_copy(table, out_ref, sem)
        copy.start()
        copy.wait()


def scatter_rows(lists, part, rows, n_dev, n_rep):
    size = lists.shape[0] // n_rep
    total, dim = part.shape
    per_part = total // (n_dev * n_rep)
    n_tok = per_part * n_dev
    return pl.pallas_call(
        functools.partial(scatter_kernel, rows.bit_length(), n_dev, n_tok, size),
        out_shape=jax.ShapeDtypeStruct((rows, dim), F32),
        grid_spec=pltpu.PrefetchScalarGridSpec(
            num_scalar_prefetch=1,
            grid=(n_dev * n_rep,),
            in_specs=[pl.BlockSpec((per_part, dim), lambda i, *_: (i, 0))],
            out_specs=pl.BlockSpec(memory_space=pl.ANY),
            scratch_shapes=[
                pltpu.VMEM((rows, dim), F32),
                pltpu.VMEM((per_part, dim), F32),
                pltpu.SemaphoreType.DMA,
            ],
        ),
        compiler_params=pltpu.CompilerParams(vmem_limit_bytes=32 << 20, dimension_semantics=("arbitrary",)),
        cost_estimate=pl.CostEstimate(
            flops=total * 1000000, bytes_accessed=4 * rows * dim + 2 * total * dim, transcendentals=0
        ),
    )(lists, part)


def sum_kernel(n, part_ref, out_ref, parts, mine, sums, send_parts, recv_parts, send_sums, recv_sums):
    me = lax.axis_index("data")
    rows = part_ref.shape[0] // n
    peers = [lax.rem(me + k, n) for k in range(1, n)]

    barrier = pltpu.get_barrier_semaphore()
    for peer in peers:
        pl.semaphore_signal(barrier, inc=1, device_id={"data": peer}, device_id_type=pl.DeviceIdType.MESH)
    pl.semaphore_wait(barrier, n - 1)

    def piece(of):
        return pl.ds(pl.multiple_of(of * rows, 8), rows)

    def send(src, slots, k, send_sem, recv_sem):
        copy = pltpu.make_async_remote_copy(
            src_ref=src,
            dst_ref=slots.at[k],
            send_sem=send_sem.at[k],
            recv_sem=recv_sem.at[k],
            device_id={"data": peers[k]},
            device_id_type=pl.DeviceIdType.MESH,
        )
        copy.start()
        return copy

    first = [send(part_ref.at[piece(peers[k])], parts, k, send_parts, recv_parts) for k in range(n - 1)]
    total = part_ref[piece(me), :]
    for k in range(n - 1):
        first[k].wait()
        total = total + parts[k]
    mine[...] = total
    out_ref[piece(me), :] = mine[...]
    second = [send(mine, sums, k, send_sums, recv_sums) for k in range(n - 1)]
    for k in range(n - 1):
        second[k].wait()
        out_ref[piece(lax.rem(me + n - 1 - k, n)), :] = sums[k]


def sum_over_data(part, n, number):
    rows, dim = part.shape[0] // n, part.shape[1]
    sems = pltpu.SemaphoreType.DMA((n - 1,))
    return pl.pallas_call(
        functools.partial(sum_kernel, n),
        out_shape=jax.ShapeDtypeStruct(part.shape, F32),
        in_specs=[pl.BlockSpec(memory_space=pltpu.VMEM)],
        out_specs=pl.BlockSpec(memory_space=pltpu.VMEM),
        scratch_shapes=[
            pltpu.VMEM((n - 1, rows, dim), F32),
            pltpu.VMEM((rows, dim), F32),
            pltpu.VMEM((n - 1, rows, dim), F32),
            sems,
            sems,
            sems,
            sems,
        ],
        compiler_params=pltpu.CompilerParams(collective_id=number, has_side_effects=True, vmem_limit_bytes=16 << 20),
        cost_estimate=pl.CostEstimate(flops=part.size * 50000, bytes_accessed=8 * part.size, transcendentals=0),
    )(part)


def pair_kernel(blocks_ref, out_ref, recv, send_sem, recv_sem):
    me = lax.axis_index("tensor")
    parity = lax.rem(me, 2)
    partner = me + 1 - 2 * parity
    n_out, rows, _ = out_ref.shape

    barrier = pltpu.get_barrier_semaphore()
    pl.semaphore_signal(barrier, inc=1, device_id={"tensor": partner}, device_id_type=pl.DeviceIdType.MESH)
    pl.semaphore_wait(barrier, 1)

    copies = []
    for k in range(n_out):
        copy = pltpu.make_async_remote_copy(
            src_ref=blocks_ref.at[2 * k + 1 - parity],
            dst_ref=recv.at[k],
            send_sem=send_sem.at[k],
            recv_sem=recv_sem.at[k],
            device_id={"tensor": partner},
            device_id_type=pl.DeviceIdType.MESH,
        )
        copy.start()
        copies.append(copy)
    for k in range(n_out):
        copies[k].wait()

        def add(i, carry, k=k):
            part = pl.ds(pl.multiple_of(i * PAIR_ROWS, PAIR_ROWS), PAIR_ROWS)
            mine = blocks_ref[2 * k + parity, part, :].astype(F32)
            out_ref[k, part, :] = (mine + recv[k, part, :].astype(F32)).astype(out_ref.dtype)
            return carry

        lax.fori_loop(0, rows // PAIR_ROWS, add, 0)


def sum_pairs(value, n_blocks, number):
    total, dim = value.shape
    n_out, rows = n_blocks // 2, total // n_blocks
    sems = pltpu.SemaphoreType.DMA((n_out,))
    out = pl.pallas_call(
        pair_kernel,
        out_shape=jax.ShapeDtypeStruct((n_out, rows, dim), value.dtype),
        in_specs=[pl.BlockSpec(memory_space=pltpu.VMEM)],
        out_specs=pl.BlockSpec(memory_space=pltpu.VMEM),
        scratch_shapes=[pltpu.VMEM((n_out, rows, dim), value.dtype), sems, sems],
        compiler_params=pltpu.CompilerParams(collective_id=number, has_side_effects=True, vmem_limit_bytes=32 << 20),
        cost_estimate=pl.CostEstimate(flops=value.size * 4000, bytes_accessed=6 * value.size, transcendentals=0),
    )(value.reshape(n_blocks, rows, dim))
    return out.reshape(n_out * rows, dim)


def solution(mesh):
    tok_spec = P(("pod", "data", "tensor"), None)
    n_dev = mesh.shape["tensor"]
    n_rep = mesh.shape["data"]

    def body(token_ids, embed_table, norm_gain, w_in, w_out, d_out):
        shard_rows, dim = embed_table.shape
        rank = lax.axis_index("tensor")
        n_tok = token_ids.shape[0]
        per_dev = n_tok // n_dev
        bounds = [0, per_dev * SPLIT[0] // sum(SPLIT), per_dev]

        cols = w_out.shape[0]
        w_both = jnp.concatenate([w_in.T, w_out], axis=0)
        w_both = with_layout_constraint(w_both, Layout(major_to_minor=(0, 1)))
        w_both = lax.all_gather(w_both, "tensor", axis=0)
        w1t = lax.optimization_barrier(w_both[:, :cols].reshape(-1, dim))
        w2 = lax.optimization_barrier(w_both[:, cols:].reshape(-1, dim))

        ids_by_dev = token_ids.reshape(n_dev, per_dev)
        gain_f32 = norm_gain.astype(F32)

        x_halves = []
        groups = [list(range(k, n_dev, 2)) for k in range(2)]
        for k in range(len(SPLIT)):
            local_ids = ids_by_dev[:, bounds[k] : bounds[k + 1]].reshape(-1) - rank * shard_rows
            is_owned = (local_ids >= 0) & (local_ids < shard_rows)
            picked = jnp.take(embed_table, jnp.where(is_owned, local_ids, 0), axis=0)
            partial_rows = jnp.where(is_owned[:, None], picked, jnp.zeros_like(picked))
            partial_rows = sum_pairs(partial_rows, n_dev, 2 + k)
            x_halves.append(
                lax.psum_scatter(partial_rows, "tensor", scatter_dimension=0, axis_index_groups=groups, tiled=True)
            )

        lists = list_owned(token_ids, shard_rows, rank, n_dev)
        lists = lax.all_gather(lists, "data", axis=0, tiled=True)

        grads, saved = [], []
        for k in range(len(SPLIT)):
            d_half = lax.slice_in_dim(d_out, bounds[k], bounds[k + 1])
            grad_hidden = lax.dot_general(d_half, w2, NT, preferred_element_type=F32)
            grad_hidden = lax.optimization_barrier(grad_hidden)
            x_half = x_halves[k]
            if k > 0:
                x_half, _ = lax.optimization_barrier((x_half, d_embed))
            x_f32 = x_half.astype(F32)
            inv_rms = lax.rsqrt(jnp.mean(x_f32 * x_f32, axis=-1, keepdims=True) + NORM_EPS)
            x_hat = x_f32 * inv_rms
            normed = (x_hat * gain_f32).astype(BF16)
            pre_gelu = lax.dot_general(normed, w1t, NT, preferred_element_type=F32).astype(BF16)
            hidden_f32, gelu_pull = jax.vjp(gelu_tanh, pre_gelu.astype(F32))
            hidden = hidden_f32.astype(BF16)
            grad_pre = gelu_pull(grad_hidden)[0].astype(BF16)
            d_normed = jnp.dot(grad_pre, w1t, preferred_element_type=F32)
            d_hat = d_normed * gain_f32
            d_norm_in = inv_rms * (d_hat - x_hat * jnp.mean(d_hat * x_hat, axis=-1, keepdims=True))
            d_embed = (d_half.astype(F32) + d_norm_in).astype(BF16)
            grads.append(d_embed)
            normed, hidden, grad_pre, _ = lax.optimization_barrier((normed, hidden, grad_pre, d_embed))
            saved.append((normed, hidden, grad_pre))
        normed, hidden, grad_pre = (lax.optimization_barrier(jnp.concatenate(v, axis=0)) for v in zip(*saved))
        x_f32 = jnp.concatenate(x_halves, axis=0).astype(F32)
        mlp_out = jnp.dot(hidden, w2, preferred_element_type=F32)
        block_out = (x_f32 + mlp_out).astype(BF16)
        grad_all = lax.all_gather(jnp.concatenate(grads, axis=0), ("data", "tensor"), axis=0, tiled=True)

        grad_w2 = lax.dot_general(hidden, d_out, TN, preferred_element_type=F32)
        grad_w1t = lax.dot_general(grad_pre, normed, TN, preferred_element_type=F32)
        grad_w2 = sum_pairs(grad_w2, n_dev, 4)
        grad_w1t = sum_pairs(grad_w1t, n_dev, 5)
        grad_w2 = lax.psum_scatter(grad_w2, "tensor", scatter_dimension=0, axis_index_groups=groups, tiled=True)
        grad_w1t = lax.psum_scatter(grad_w1t, "tensor", scatter_dimension=0, axis_index_groups=groups, tiled=True)
        grad_w2 = sum_over_data(grad_w2, n_rep, 0)
        grad_w1t = sum_over_data(grad_w1t, n_rep, 1)
        grad_table = scatter_rows(lists, grad_all, shard_rows, n_dev, n_rep)
        return block_out, grad_table, grad_w1t.T, grad_w2

    return jax.shard_map(
        body,
        mesh=mesh,
        in_specs=(P(("pod", "data")), P("tensor", None), P(None), P(None, "tensor"), P("tensor", None), tok_spec),
        out_specs=(tok_spec, P(("pod", "tensor"), None), P("pod", "tensor"), P(("pod", "tensor"), None)),
        check_vma=False,
    )
```
